32 devices in a mesh: band: 2 (over x), row: 16 (over z, y, core).
Axes of the slice: x: 2, y: 2, z: 4, core: 2. Of those that a mesh axis runs over, the one named last changes fastest.
Arguments:
- shot_traces: bfloat16 [16384, 4096], P(('band', 'row')), parts along dimension 0, may hold values from -6 to 6
- source_cell: int32 [16384], P(('band', 'row')), parts along dimension 0, may hold values from 0 to 127
- receiver_cell: int32 [16384], P(('band', 'row')), parts along dimension 0, may hold values from 0 to 127
- band_order: int32 [64], P('band'), parts along dimension 0, may hold values from 0 to 31, each once
Outputs:
- next_grid: float32 [64, 2, 128, 128], P(('band', 'row')), parts along dimension 0
The draws below stay inside these ranges and needn't reach their ends.
There are 2 independent parts, one for each index of `band`. The reference program is written for one: setup_inputs(seed, part) draws one part's arguments, and reference() takes and returns one part's arrays. A program takes and returns all parts, laid end to end along the dimension named above; each array names one. Nothing has to cross between parts.
Inputs may be any that keep to these rules, and one draw needn't show every extreme that they name: `band_order`: a permutation of 0 to 31.
All inputs are finite; a program needn't handle non-finite values.
Results may differ from the reference program's by a relative error of at most 0.0037.
Values may be sent and summed in bfloat16 or wider, within the bound.
A program may use at most 64 MiB of HBM per device.

```python
import math
import jax
import jax.numpy as jnp
from jax import lax

NT = 4096
FLO = 64
SC = 128
RC = 128
NFB = 32
TRACES = 8192


def place_ends(drawn, stream_key, smallest, top_value):
    dims = drawn.shape
    index_at = [jax.random.randint(jax.random.fold_in(stream_key, axis), (), 0, dims[axis]) for axis in range(len(dims))]
    drawn = drawn.at[tuple(index_at)].set(smallest)
    longest = dims.index(max(dims))
    index_at[longest] = (index_at[longest] + 1) % dims[longest]
    return drawn.at[tuple(index_at)].set(top_value)


def shard_levels(rng, shape, split, smallest, top_value):
    def one(axis_at, shards_of):
        heights = jax.random.uniform(jax.random.fold_in(jax.random.fold_in(rng, 6), axis_at), (shards_of,), jnp.float32, smallest / len(split), top_value / len(split))
        return jnp.repeat(jnp.exp(heights), shape[axis_at] // shards_of).reshape((-1,) + (1,) * (len(shape) - axis_at - 1))

    loudness = one(*split[0])
    for cut in split[1:]:
        loudness = loudness * one(*cut)
    return loudness


def gaussian(own_key, extent, scale, limit, shards=(), held_as=jnp.bfloat16):
    result = jax.random.normal(own_key, extent, jnp.float32) * scale
    if len(shards) > 0:
        result = shard_levels(own_key, extent, shards, -0.22, 0.18) * result
    return jnp.clip(result, min=-limit, max=limit).astype(held_as)


def setup_inputs(seed: int = 0, part: int = 0) -> dict:
    streams_of = jax.random.split(jax.random.key(seed), 5)
    part_splits = jax.random.split(jax.random.fold_in(streams_of[4], part), 5)
    shot_traces = gaussian(part_splits[0], (TRACES, NT), 1.0, 6.0, ((0, 16),))
    source_cell = place_ends(jax.random.randint(part_splits[1], (TRACES,), 0, SC), jax.random.fold_in(part_splits[1], 1), 0, SC - 1).astype(jnp.int32)
    receiver_cell = place_ends(jax.random.randint(part_splits[2], (TRACES,), 0, RC), jax.random.fold_in(part_splits[2], 1), 0, RC - 1).astype(jnp.int32)
    band_order = jax.random.permutation(part_splits[3], NFB).astype(jnp.int32)
    return dict(shot_traces=shot_traces, source_cell=source_cell, receiver_cell=receiver_cell, band_order=band_order)


def reference(shot_traces, source_cell, receiver_cell, band_order):
    high = lax.Precision.HIGHEST
    bins = (FLO + band_order).astype(jnp.int32)
    samples = jnp.arange(NT, dtype=jnp.int32)
    phase = samples[:, None] * bins[None, :] % NT
    angle = 2.0 * math.pi * phase.astype(jnp.float32) / NT
    scale = 1.0 / math.sqrt(NT)
    table = jnp.concatenate([jnp.cos(angle) * scale, -jnp.sin(angle) * scale], axis=1).astype(jnp.bfloat16)
    spectra = jnp.dot(shot_traces.astype(jnp.float32), table.astype(jnp.float32), precision=high).astype(jnp.bfloat16)
    cell_ids = (source_cell * RC + receiver_cell).astype(jnp.int32)
    stack = jax.ops.segment_sum(spectra.astype(jnp.float32), cell_ids, num_segments=SC * RC)
    counts = jax.ops.segment_sum(jnp.ones(cell_ids.shape, jnp.float32), cell_ids, num_segments=SC * RC)
    stack = stack.reshape(SC, RC, 2, NFB).transpose(3, 2, 0, 1)
    next_grid = stack / jnp.maximum(counts.reshape(SC, RC), 1.0)[None, None, :, :]
    return next_grid
```

```python
import functools
import math

import jax
import jax.numpy as jnp
import ml_dtypes
import numpy as np
from jax import lax
from jax.experimental import pallas as pl
from jax.experimental.pallas import tpu as pltpu
from jax.sharding import PartitionSpec as P

FLO = 64
SC = 128
RC = 128
NCHUNK = 2
BF = jnp.bfloat16
F32 = jnp.float32
NT_DIMS = (((1,), (1,)), ((), ()))
TN_DIMS = (((0,), (0,)), ((), ()))


def natural_table(samples_count, band_size):
    bins = FLO + np.arange(band_size)
    phase = (bins[:, None] * np.arange(samples_count)[None, :]) % samples_count
    angle = 2.0 * math.pi * phase / samples_count
    scale = 1.0 / math.sqrt(samples_count)
    table = np.stack([np.cos(angle) * scale, -np.sin(angle) * scale], axis=1)
    return table.reshape(2 * band_size, samples_count).astype(np.float32).astype(ml_dtypes.bfloat16)


def kernel(
    n,
    traces_hbm,
    source_hbm,
    receiver_hbm,
    order_hbm,
    table_hbm,
    out_ref,
    traces,
    source,
    receiver,
    order,
    table,
    lhs,
    cells_out,
    cells_in,
    send,
    recv,
    source_hot,
    receiver_hot,
    counts,
    stack,
    load_sem,
    traces_sem,
    cell_send_sem,
    cell_recv_sem,
    send_sem,
    recv_sem,
    own_sem,
):
    me = lax.axis_index("row")
    chunk = traces.shape[1]
    rows, samples_count = table.shape
    channels = send.shape[2]

    def load(at, src, dst):
        return pltpu.make_async_copy(src, dst, load_sem.at[at])

    loads = [
        load(0, source_hbm, source),
        load(1, receiver_hbm, receiver),
        load(2, order_hbm, order),
        load(3, table_hbm, table),
    ]
    for copy in loads:
        copy.start()
    trace_loads = [
        pltpu.make_async_copy(
            traces_hbm.at[pl.ds(c * chunk, chunk)], traces.at[c], traces_sem.at[c]
        )
        for c in range(NCHUNK)
    ]
    for copy in trace_loads:
        copy.start()

    barrier = pltpu.get_barrier_semaphore()

    def greet(i, carry):
        pl.semaphore_signal(barrier, inc=1, device_id={"row": lax.rem(me + i, n)})
        return carry

    lax.fori_loop(1, n, greet, 0)

    loads[0].wait()
    loads[1].wait()
    cells_out[...] = source[...] * RC + receiver[...]

    loads[2].wait()
    band_size = rows // 2
    spread = (
        lax.broadcasted_iota(jnp.int32, (band_size, rows), 0)
        == lax.broadcasted_iota(jnp.int32, (band_size, rows), 1) // 2
    ).astype(BF)
    bins = jnp.broadcast_to(order[...].astype(F32), (8, band_size)).astype(BF)
    wanted = jnp.dot(bins, spread, preferred_element_type=F32)[0:1]
    part = lax.broadcasted_iota(jnp.int32, (1, rows), 1) % 2
    wanted = 2.0 * wanted + part.astype(F32)
    held = lax.broadcasted_iota(jnp.int32, (rows, rows), 0).astype(F32)
    pick = (held == wanted).astype(F32).astype(BF)
    loads[3].wait()
    for at in range(0, samples_count, 1024):
        cut = pl.ds(at, 1024)
        lhs[:, cut] = lax.dot_general(
            pick, table[:, cut], TN_DIMS, preferred_element_type=F32
        ).astype(BF)

    pl.semaphore_wait(barrier, n - 1)

    def cell_copy(peer, slot):
        return pltpu.make_async_remote_copy(
            src_ref=cells_out,
            dst_ref=cells_in.at[slot],
            send_sem=cell_send_sem.at[peer],
            recv_sem=cell_recv_sem.at[slot],
            device_id={"row": peer},
        )

    def send_cells(i, carry):
        cell_copy(lax.rem(me + i, n), me).start()
        return carry

    lax.fori_loop(1, n, send_cells, 0)
    own_cells = pltpu.make_async_copy(cells_out, cells_in.at[me], own_sem.at[NCHUNK])
    own_cells.start()

    def value_copy(c, peer, slot):
        return pltpu.make_async_remote_copy(
            src_ref=send.at[c, peer],
            dst_ref=recv.at[c, slot],
            send_sem=send_sem.at[c, peer],
            recv_sem=recv_sem.at[c, slot],
            device_id={"row": peer},
        )

    own_values = []
    for c in range(NCHUNK):
        trace_loads[c].wait()
        spectra = lax.dot_general(
            lhs[...], traces[c], NT_DIMS, preferred_element_type=F32
        )
        send[c] = spectra.reshape(n, channels, chunk).astype(BF)

        def send_values(i, carry, c=c):
            value_copy(c, lax.rem(me + i, n), me).start()
            return carry

        lax.fori_loop(1, n, send_values, 0)
        own = pltpu.make_async_copy(send.at[c, me], recv.at[c, me], own_sem.at[c])
        own.start()
        own_values.append(own)

    per_device = cells_out.shape[1]
    cell_at = lax.broadcasted_iota(jnp.int32, (SC, per_device), 0)
    counts[...] = jnp.zeros_like(counts)

    def hot(src):
        cell = cells_in[src]
        s_hot = (cell_at == cell // RC).astype(F32).astype(BF)
        r_hot = (cell_at == cell % RC).astype(F32).astype(BF)
        source_hot[src] = s_hot
        receiver_hot[src] = r_hot
        counts[...] += lax.dot_general(s_hot, r_hot, NT_DIMS, preferred_element_type=F32)

    own_cells.wait()
    hot(me)

    def hot_step(i, carry):
        src = lax.rem(me + n - i, n)
        cell_copy(src, src).wait_recv()
        hot(src)
        return carry

    lax.fori_loop(1, n, hot_step, 0)

    stack[...] = jnp.zeros_like(stack)

    def add(c, src):
        cut = pl.ds(c * chunk, chunk)
        s_hot = source_hot[src, :, cut]
        r_hot = receiver_hot[src, :, cut]
        values = recv[c, src]
        weighted = jnp.concatenate(
            [r_hot * values[m : m + 1, :] for m in range(channels)], axis=0
        )
        stack[...] += lax.dot_general(s_hot, weighted, NT_DIMS, preferred_element_type=F32)

    for c in range(NCHUNK):
        own_values[c].wait()
        add(c, me)

        def add_step(i, carry, c=c):
            src = lax.rem(me + n - i, n)
            value_copy(c, src, src).wait_recv()
            add(c, src)
            return carry

        lax.fori_loop(1, n, add_step, 0)

    scale = 1.0 / jnp.maximum(counts[...], 1.0)
    for m in range(channels):
        out_ref[m // 2, m % 2] = stack[:, m * RC : (m + 1) * RC] * scale

    def drain(i, carry):
        peer = lax.rem(me + i, n)
        cell_copy(peer, me).wait_send()
        for c in range(NCHUNK):
            value_copy(c, peer, me).wait_send()
        return carry

    lax.fori_loop(1, n, drain, 0)


def local(n, shot_traces, source_cell, receiver_cell, band_order):
    local_traces, samples_count = shot_traces.shape
    band_size = band_order.shape[0]
    own_slots = band_size // n
    rows = 2 * band_size
    channels = 2 * own_slots
    chunk = local_traces // NCHUNK
    table = jnp.asarray(natural_table(samples_count, band_size))
    anywhere = pl.BlockSpec(memory_space=pltpu.HBM)
    return pl.pallas_call(
        functools.partial(kernel, n),
        out_shape=jax.ShapeDtypeStruct((own_slots, 2, SC, RC), F32),
        in_specs=[anywhere] * 5,
        out_specs=pl.BlockSpec(memory_space=pltpu.VMEM),
        scratch_shapes=[
            pltpu.VMEM((NCHUNK, chunk, samples_count), BF),
            pltpu.VMEM((1, local_traces), jnp.int32),
            pltpu.VMEM((1, local_traces), jnp.int32),
            pltpu.VMEM((1, band_size), jnp.int32),
            pltpu.VMEM((rows, samples_count), BF),
            pltpu.VMEM((rows, samples_count), BF),
            pltpu.VMEM((1, local_traces), jnp.int32),
            pltpu.VMEM((n, 1, local_traces), jnp.int32),
            pltpu.VMEM((NCHUNK, n, channels, chunk), BF),
            pltpu.VMEM((NCHUNK, n, channels, chunk), BF),
            pltpu.VMEM((n, SC, local_traces), BF),
            pltpu.VMEM((n, RC, local_traces), BF),
            pltpu.VMEM((SC, RC), F32),
            pltpu.VMEM((SC, channels * RC), F32),
            pltpu.SemaphoreType.DMA((4,)),
            pltpu.SemaphoreType.DMA((NCHUNK,)),
            pltpu.SemaphoreType.DMA((n,)),
            pltpu.SemaphoreType.DMA((n,)),
            pltpu.SemaphoreType.DMA((NCHUNK, n)),
            pltpu.SemaphoreType.DMA((NCHUNK, n)),
            pltpu.SemaphoreType.DMA((NCHUNK + 1,)),
        ],
        compiler_params=pltpu.CompilerParams(
            collective_id=0, has_side_effects=True, vmem_limit_bytes=48 * 1024 * 1024
        ),
    )(
        shot_traces,
        source_cell.reshape(1, local_traces),
        receiver_cell.reshape(1, local_traces),
        band_order.reshape(1, band_size),
        table,
    )


def solution(mesh):
    placed = (P(("band", "row"), None), P(("band", "row")), P(("band", "row")), P("band"))
    return jax.shard_map(
        functools.partial(local, mesh.shape["row"]),
        mesh=mesh,
        in_specs=placed,
        out_specs=P(("band", "row"), None, None, None),
        check_vma=False,
    )
```

```python
import functools
import math

import jax
import jax.numpy as jnp
import ml_dtypes
import numpy as np
from jax import lax
from jax.experimental import pallas as pl
from jax.experimental.pallas import tpu as pltpu
from jax.sharding import PartitionSpec as P

FLO = 64
SC = 128
RC = 128
NCHUNK = 2
GROUP = 4
BF = jnp.bfloat16
F32 = jnp.float32
NT_DIMS = (((1,), (1,)), ((), ()))
TN_DIMS = (((0,), (0,)), ((), ()))


def natural_table(samples_count, band_size):
    bins = FLO + np.arange(band_size)
    phase = (bins[:, None] * np.arange(samples_count)[None, :]) % samples_count
    angle = 2.0 * math.pi * phase / samples_count
    scale = 1.0 / math.sqrt(samples_count)
    table = np.stack([np.cos(angle) * scale, -np.sin(angle) * scale], axis=1)
    return table.reshape(2 * band_size, samples_count).astype(np.float32).astype(ml_dtypes.bfloat16)


def kernel(
    n,
    traces_hbm,
    source_hbm,
    receiver_hbm,
    order_hbm,
    table_hbm,
    out_ref,
    traces,
    source,
    receiver,
    order,
    table,
    lhs,
    cells_out,
    cells_in,
    send,
    recv,
    stack,
    load_sem,
    traces_sem,
    cell_send_sem,
    cell_recv_sem,
    send_sem,
    recv_sem,
    own_sem,
):
    me = lax.axis_index("row")
    chunk = traces.shape[1]
    rows, samples_count = table.shape
    channels = send.shape[2]

    def load(at, src, dst):
        return pltpu.make_async_copy(src, dst, load_sem.at[at])

    loads = [
        load(0, source_hbm, source),
        load(1, receiver_hbm, receiver),
        load(2, order_hbm, order),
        load(3, table_hbm, table),
    ]
    for copy in loads:
        copy.start()
    trace_loads = [
        pltpu.make_async_copy(
            traces_hbm.at[pl.ds(c * chunk, chunk)], traces.at[c], traces_sem.at[c]
        )
        for c in range(NCHUNK)
    ]
    for copy in trace_loads:
        copy.start()

    barrier = pltpu.get_barrier_semaphore()

    def greet(i, carry):
        pl.semaphore_signal(barrier, inc=1, device_id={"row": lax.rem(me + i, n)})
        return carry

    lax.fori_loop(1, n, greet, 0)

    loads[0].wait()
    loads[1].wait()
    cells_out[...] = source[...] * RC + receiver[...]

    loads[2].wait()
    band_size = rows // 2
    spread = (
        lax.broadcasted_iota(jnp.int32, (band_size, rows), 0)
        == lax.broadcasted_iota(jnp.int32, (band_size, rows), 1) // 2
    ).astype(BF)
    bins = jnp.broadcast_to(order[...].astype(F32), (8, band_size)).astype(BF)
    wanted = jnp.dot(bins, spread, preferred_element_type=F32)[0:1]
    part = lax.broadcasted_iota(jnp.int32, (1, rows), 1) % 2
    wanted = 2.0 * wanted + part.astype(F32)
    held = lax.broadcasted_iota(jnp.int32, (rows, rows), 0).astype(F32)
    pick = (held == wanted).astype(F32).astype(BF)
    loads[3].wait()
    for at in range(0, samples_count, 1024):
        cut = pl.ds(at, 1024)
        lhs[:, cut] = lax.dot_general(
            pick, table[:, cut], TN_DIMS, preferred_element_type=F32
        ).astype(BF)

    def cell_copy(peer, slot):
        return pltpu.make_async_remote_copy(
            src_ref=cells_out,
            dst_ref=cells_in.at[slot],
            send_sem=cell_send_sem.at[peer],
            recv_sem=cell_recv_sem.at[slot],
            device_id={"row": peer},
        )

    def value_copy(c, peer, slot):
        return pltpu.make_async_remote_copy(
            src_ref=send.at[c, peer],
            dst_ref=recv.at[c, slot],
            send_sem=send_sem.at[c, peer],
            recv_sem=recv_sem.at[c, slot],
            device_id={"row": peer},
        )

    own_values = []
    for c in range(NCHUNK):
        trace_loads[c].wait()
        spectra = lax.dot_general(
            lhs[...], traces[c], NT_DIMS, preferred_element_type=F32
        )
        send[c] = spectra.reshape(n, channels, chunk).astype(BF)

        if c == 0:
            pl.semaphore_wait(barrier, n - 1)

            def send_cells(i, carry):
                cell_copy(lax.rem(me + i, n), me).start()
                return carry

            lax.fori_loop(1, n, send_cells, 0)
            own_cells = pltpu.make_async_copy(cells_out, cells_in.at[me], own_sem.at[NCHUNK])
            own_cells.start()

        def send_values(i, carry, c=c):
            value_copy(c, lax.rem(me + i, n), me).start()
            return carry

        lax.fori_loop(1, n, send_values, 0)
        own = pltpu.make_async_copy(send.at[c, me], recv.at[c, me], own_sem.at[c])
        own.start()
        own_values.append(own)

    cell_at = lax.broadcasted_iota(jnp.int32, (SC, chunk), 0)
    stack[...] = jnp.zeros_like(stack)

    def add(sources):
        s_parts, w_parts = [], []
        for src in sources:
            for c in range(NCHUNK):
                cell = cells_in[src, :, c * chunk : (c + 1) * chunk]
                s_parts.append((cell_at == cell // RC).astype(F32).astype(BF))
                r_hot = (cell_at == cell % RC).astype(F32).astype(BF)
                values = recv[c, src]
                w_parts.append(
                    jnp.concatenate(
                        [r_hot * values[m : m + 1, :] for m in range(channels)] + [r_hot],
                        axis=0,
                    )
                )
        stack[...] += lax.dot_general(
            jnp.concatenate(s_parts, axis=1),
            jnp.concatenate(w_parts, axis=1),
            NT_DIMS,
            preferred_element_type=F32,
        )

    def arrive(src):
        cell_copy(src, src).wait_recv()
        for c in range(NCHUNK):
            value_copy(c, src, src).wait_recv()

    own_cells.wait()
    for own in own_values:
        own.wait()
    group = [lax.rem(me + n - k, n) for k in range(GROUP)]
    for src in group[1:]:
        arrive(src)
    add(group)

    def add_step(g, carry):
        sources = [lax.rem(me + n - (g * GROUP + k), n) for k in range(GROUP)]
        for src in sources:
            arrive(src)
        add(sources)
        return carry

    lax.fori_loop(1, n // GROUP, add_step, 0)

    scale = 1.0 / jnp.maximum(stack[:, channels * RC :], 1.0)
    for m in range(channels):
        out_ref[m // 2, m % 2] = stack[:, m * RC : (m + 1) * RC] * scale

    def drain(i, carry):
        peer = lax.rem(me + i, n)
        cell_copy(peer, me).wait_send()
        for c in range(NCHUNK):
            value_copy(c, peer, me).wait_send()
        return carry

    lax.fori_loop(1, n, drain, 0)


def local(n, shot_traces, source_cell, receiver_cell, band_order):
    local_traces, samples_count = shot_traces.shape
    band_size = band_order.shape[0]
    own_slots = band_size // n
    rows = 2 * band_size
    channels = 2 * own_slots
    chunk = local_traces // NCHUNK
    table = jnp.asarray(natural_table(samples_count, band_size))
    anywhere = pl.BlockSpec(memory_space=pltpu.HBM)
    return pl.pallas_call(
        functools.partial(kernel, n),
        out_shape=jax.ShapeDtypeStruct((own_slots, 2, SC, RC), F32),
        in_specs=[anywhere] * 5,
        out_specs=pl.BlockSpec(memory_space=pltpu.VMEM),
        scratch_shapes=[
            pltpu.VMEM((NCHUNK, chunk, samples_count), BF),
            pltpu.VMEM((1, local_traces), jnp.int32),
            pltpu.VMEM((1, local_traces), jnp.int32),
            pltpu.VMEM((1, band_size), jnp.int32),
            pltpu.VMEM((rows, samples_count), BF),
            pltpu.VMEM((rows, samples_count), BF),
            pltpu.VMEM((1, local_traces), jnp.int32),
            pltpu.VMEM((n, 1, local_traces), jnp.int32),
            pltpu.VMEM((NCHUNK, n, channels, chunk), BF),
            pltpu.VMEM((NCHUNK, n, channels, chunk), BF),
            pltpu.VMEM((SC, (channels + 1) * RC), F32),
            pltpu.SemaphoreType.DMA((4,)),
            pltpu.SemaphoreType.DMA((NCHUNK,)),
            pltpu.SemaphoreType.DMA((n,)),
            pltpu.SemaphoreType.DMA((n,)),
            pltpu.SemaphoreType.DMA((NCHUNK, n)),
            pltpu.SemaphoreType.DMA((NCHUNK, n)),
            pltpu.SemaphoreType.DMA((NCHUNK + 1,)),
        ],
        compiler_params=pltpu.CompilerParams(
            collective_id=0, has_side_effects=True, vmem_limit_bytes=64 * 1024 * 1024 - 65536
        ),
    )(
        shot_traces,
        source_cell.reshape(1, local_traces),
        receiver_cell.reshape(1, local_traces),
        band_order.reshape(1, band_size),
        table,
    )


def solution(mesh):
    placed = (P(("band", "row"), None), P(("band", "row")), P(("band", "row")), P("band"))
    return jax.shard_map(
        functools.partial(local, mesh.shape["row"]),
        mesh=mesh,
        in_specs=placed,
        out_specs=P(("band", "row"), None, None, None),
        check_vma=False,
    )
```

```python
import functools
import math

import jax
import jax.numpy as jnp
import ml_dtypes
import numpy as np
from jax import lax
from jax.experimental import pallas as pl
from jax.experimental.pallas import tpu as pltpu
from jax.sharding import PartitionSpec as P

FLO = 64
SC = 128
RC = 128
NCHUNK = 2
GROUP = 4
BF = jnp.bfloat16
F32 = jnp.float32
NT_DIMS = (((1,), (1,)), ((), ()))
TN_DIMS = (((0,), (0,)), ((), ()))


def natural_table(samples_count, band_size):
    bins = FLO + np.arange(band_size)
    phase = (bins[:, None] * np.arange(samples_count)[None, :]) % samples_count
    angle = 2.0 * math.pi * phase / samples_count
    scale = 1.0 / math.sqrt(samples_count)
    table = np.stack([np.cos(angle) * scale, -np.sin(angle) * scale], axis=1)
    return table.reshape(2 * band_size, samples_count).astype(np.float32).astype(ml_dtypes.bfloat16)


def kernel(
    n,
    traces_hbm,
    source_hbm,
    receiver_hbm,
    order_hbm,
    table_hbm,
    out_ref,
    traces,
    source,
    receiver,
    order,
    table,
    lhs,
    cells_out,
    cells_in,
    send,
    recv,
    stack,
    load_sem,
    traces_sem,
    cell_send_sem,
    cell_recv_sem,
    send_sem,
    recv_sem,
    own_sem,
):
    me = lax.axis_index("row")
    chunk = traces.shape[1]
    rows, samples_count = table.shape
    channels = send.shape[2]

    def load(at, src, dst):
        return pltpu.make_async_copy(src, dst, load_sem.at[at])

    loads = [
        load(0, source_hbm, source),
        load(1, receiver_hbm, receiver),
        load(2, order_hbm, order),
        load(3, table_hbm, table),
    ]
    for copy in loads:
        copy.start()
    trace_loads = [
        pltpu.make_async_copy(
            traces_hbm.at[pl.ds(c * chunk, chunk)], traces.at[c], traces_sem.at[c]
        )
        for c in range(NCHUNK)
    ]
    for copy in trace_loads:
        copy.start()

    barrier = pltpu.get_barrier_semaphore()

    def greet(i, carry):
        pl.semaphore_signal(barrier, inc=1, device_id={"row": lax.rem(me + i, n)})
        return carry

    lax.fori_loop(1, n, greet, 0)

    loads[0].wait()
    loads[1].wait()
    cells_out[...] = source[...] * RC + receiver[...]

    loads[2].wait()
    band_size = rows // 2
    spread = (
        lax.broadcasted_iota(jnp.int32, (band_size, rows), 0)
        == lax.broadcasted_iota(jnp.int32, (band_size, rows), 1) // 2
    ).astype(BF)
    bins = jnp.broadcast_to(order[...].astype(F32), (8, band_size)).astype(BF)
    wanted = jnp.dot(bins, spread, preferred_element_type=F32)[0:1]
    part = lax.broadcasted_iota(jnp.int32, (1, rows), 1) % 2
    wanted = 2.0 * wanted + part.astype(F32)
    held = lax.broadcasted_iota(jnp.int32, (rows, rows), 0).astype(F32)
    pick = (held == wanted).astype(F32).astype(BF)
    loads[3].wait()
    for at in range(0, samples_count, 1024):
        cut = pl.ds(at, 1024)
        lhs[:, cut] = lax.dot_general(
            pick, table[:, cut], TN_DIMS, preferred_element_type=F32
        ).astype(BF)

    def cell_copy(peer, slot):
        return pltpu.make_async_remote_copy(
            src_ref=cells_out,
            dst_ref=cells_in.at[slot],
            send_sem=cell_send_sem.at[peer],
            recv_sem=cell_recv_sem.at[slot],
            device_id={"row": peer},
        )

    def value_copy(c, peer, slot):
        return pltpu.make_async_remote_copy(
            src_ref=send.at[c, peer],
            dst_ref=recv.at[c, slot],
            send_sem=send_sem.at[c, peer],
            recv_sem=recv_sem.at[c, slot],
            device_id={"row": peer},
        )

    own_values = []
    for c in range(NCHUNK):
        trace_loads[c].wait()
        spectra = lax.dot_general(
            lhs[...], traces[c], NT_DIMS, preferred_element_type=F32
        )
        send[c] = spectra.reshape(n, channels, chunk).astype(BF)

        if c == 0:
            pl.semaphore_wait(barrier, n - 1)

            def send_cells(i, carry):
                cell_copy(lax.rem(me + i, n), me).start()
                return carry

            lax.fori_loop(1, n, send_cells, 0)
            own_cells = pltpu.make_async_copy(cells_out, cells_in.at[me], own_sem.at[NCHUNK])
            own_cells.start()

        def send_values(i, carry, c=c):
            value_copy(c, lax.rem(me + i, n), me).start()
            return carry

        lax.fori_loop(1, n, send_values, 0)
        own = pltpu.make_async_copy(send.at[c, me], recv.at[c, me], own_sem.at[c])
        own.start()
        own_values.append(own)

    cell_at = lax.broadcasted_iota(jnp.int32, (SC, chunk), 0)
    stack[...] = jnp.zeros_like(stack)

    def add(sources):
        s_parts, w_parts = [], []
        for src in sources:
            for c in range(NCHUNK):
                cell = cells_in[src, :, c * chunk : (c + 1) * chunk]
                s_parts.append((cell_at == cell // RC).astype(F32).astype(BF))
                r_hot = (cell_at == cell % RC).astype(F32).astype(BF)
                values = recv[c, src]
                w_parts.append(
                    jnp.concatenate(
                        [r_hot * values[m : m + 1, :] for m in range(channels)] + [r_hot],
                        axis=0,
                    )
                )
        stack[...] += lax.dot_general(
            jnp.concatenate(s_parts, axis=1),
            jnp.concatenate(w_parts, axis=1),
            NT_DIMS,
            preferred_element_type=F32,
        )

    def arrive(src):
        cell_copy(src, src).wait_recv()
        for c in range(NCHUNK):
            value_copy(c, src, src).wait_recv()

    own_cells.wait()
    for own in own_values:
        own.wait()
    group = [lax.rem(me + n - k, n) for k in range(GROUP)]
    for src in group[1:]:
        arrive(src)
    add(group)

    def add_step(g, carry):
        sources = [lax.rem(me + n - (g * GROUP + k), n) for k in range(GROUP)]
        for src in sources:
            arrive(src)
        add(sources)
        return carry

    lax.fori_loop(1, n // GROUP, add_step, 0)

    scale = 1.0 / jnp.maximum(stack[:, channels * RC :], 1.0)
    for m in range(channels):
        out_ref[m // 2, m % 2] = stack[:, m * RC : (m + 1) * RC] * scale

    def drain(i, carry):
        peer = lax.rem(me + i, n)
        cell_copy(peer, me).wait_send()
        for c in range(NCHUNK):
            value_copy(c, peer, me).wait_send()
        return carry

    lax.fori_loop(1, n, drain, 0)


def local(n, shot_traces, source_cell, receiver_cell, band_order):
    local_traces, samples_count = shot_traces.shape
    band_size = band_order.shape[0]
    own_slots = band_size // n
    rows = 2 * band_size
    channels = 2 * own_slots
    chunk = local_traces // NCHUNK
    table = jnp.asarray(natural_table(samples_count, band_size))
    anywhere = pl.BlockSpec(memory_space=pltpu.HBM)
    return pl.pallas_call(
        functools.partial(kernel, n),
        out_shape=pltpu.VMEM((own_slots, 2, SC, RC), F32),
        in_specs=[anywhere] * 5,
        out_specs=pl.BlockSpec(memory_space=pltpu.VMEM),
        scratch_shapes=[
            pltpu.VMEM((NCHUNK, chunk, samples_count), BF),
            pltpu.VMEM((1, local_traces), jnp.int32),
            pltpu.VMEM((1, local_traces), jnp.int32),
            pltpu.VMEM((1, band_size), jnp.int32),
            pltpu.VMEM((rows, samples_count), BF),
            pltpu.VMEM((rows, samples_count), BF),
            pltpu.VMEM((1, local_traces), jnp.int32),
            pltpu.VMEM((n, 1, local_traces), jnp.int32),
            pltpu.VMEM((NCHUNK, n, channels, chunk), BF),
            pltpu.VMEM((NCHUNK, n, channels, chunk), BF),
            pltpu.VMEM((SC, (channels + 1) * RC), F32),
            pltpu.SemaphoreType.DMA((4,)),
            pltpu.SemaphoreType.DMA((NCHUNK,)),
            pltpu.SemaphoreType.DMA((n,)),
            pltpu.SemaphoreType.DMA((n,)),
            pltpu.SemaphoreType.DMA((NCHUNK, n)),
            pltpu.SemaphoreType.DMA((NCHUNK, n)),
            pltpu.SemaphoreType.DMA((NCHUNK + 1,)),
        ],
        compiler_params=pltpu.CompilerParams(
            collective_id=0, has_side_effects=True, vmem_limit_bytes=64 * 1024 * 1024 - 65536 - 1024 * 1024
        ),
    )(
        shot_traces,
        source_cell.reshape(1, local_traces),
        receiver_cell.reshape(1, local_traces),
        band_order.reshape(1, band_size),
        table,
    )


def solution(mesh):
    placed = (P(("band", "row"), None), P(("band", "row")), P(("band", "row")), P("band"))
    return jax.shard_map(
        functools.partial(local, mesh.shape["row"]),
        mesh=mesh,
        in_specs=placed,
        out_specs=P(("band", "row"), None, None, None),
        check_vma=False,
    )
```

```python
import functools
import math

import jax
import jax.numpy as jnp
import ml_dtypes
import numpy as np
from jax import lax
from jax.experimental import pallas as pl
from jax.experimental.pallas import tpu as pltpu
from jax.sharding import PartitionSpec as P

FLO = 64
SC = 128
RC = 128
PIECES = 8
GROUP = 4
BF = jnp.bfloat16
F32 = jnp.float32
NT_DIMS = (((1,), (1,)), ((), ()))
TN_DIMS = (((0,), (0,)), ((), ()))


def natural_table(samples_count, band_size):
    bins = FLO + np.arange(band_size)
    phase = (bins[:, None] * np.arange(samples_count)[None, :]) % samples_count
    angle = 2.0 * math.pi * phase / samples_count
    scale = 1.0 / math.sqrt(samples_count)
    table = np.stack([np.cos(angle) * scale, -np.sin(angle) * scale], axis=1)
    return table.reshape(2 * band_size, samples_count).astype(np.float32).astype(ml_dtypes.bfloat16)


def kernel(
    n,
    traces_hbm,
    source_hbm,
    receiver_hbm,
    order_hbm,
    table_hbm,
    out_ref,
    traces,
    source,
    receiver,
    order,
    table,
    lhs,
    cells_out,
    cells_in,
    send,
    recv,
    stack,
    load_sem,
    traces_sem,
    cell_send_sem,
    cell_recv_sem,
    send_sem,
    recv_sem,
    own_sem,
):
    me = lax.axis_index("row")
    piece = traces.shape[2]
    per_device = traces.shape[1]
    rows, samples_count = table.shape
    channels = send.shape[1]

    def load(at, src, dst):
        return pltpu.make_async_copy(src, dst, load_sem.at[at])

    loads = [
        load(0, source_hbm, source),
        load(1, receiver_hbm, receiver),
        load(2, order_hbm, order),
        load(3, table_hbm, table),
    ]
    for copy in loads:
        copy.start()
    trace_loads = [
        pltpu.make_async_copy(
            traces_hbm.at[:, pl.ds(c * piece, piece)], traces.at[c], traces_sem.at[c]
        )
        for c in range(PIECES)
    ]
    for copy in trace_loads:
        copy.start()

    barrier = pltpu.get_barrier_semaphore()

    def greet(i, carry):
        pl.semaphore_signal(barrier, inc=1, device_id={"row": lax.rem(me + i, n)})
        return carry

    lax.fori_loop(1, n, greet, 0)

    loads[0].wait()
    loads[1].wait()
    cells_out[...] = source[...] * RC + receiver[...]

    loads[2].wait()
    band_size = rows // 2
    spread = (
        lax.broadcasted_iota(jnp.int32, (band_size, rows), 0)
        == lax.broadcasted_iota(jnp.int32, (band_size, rows), 1) // 2
    ).astype(BF)
    bins = jnp.broadcast_to(order[...].astype(F32), (8, band_size)).astype(BF)
    wanted = jnp.dot(bins, spread, preferred_element_type=F32)[0:1]
    part = lax.broadcasted_iota(jnp.int32, (1, rows), 1) % 2
    wanted = 2.0 * wanted + part.astype(F32)
    held = lax.broadcasted_iota(jnp.int32, (rows, rows), 0).astype(F32)
    pick = (held == wanted).astype(F32).astype(BF)
    loads[3].wait()
    for at in range(0, samples_count, 1024):
        cut = pl.ds(at, 1024)
        lhs[:, cut] = lax.dot_general(
            pick, table[:, cut], TN_DIMS, preferred_element_type=F32
        ).astype(BF)

    def cell_copy(peer, slot):
        return pltpu.make_async_remote_copy(
            src_ref=cells_out,
            dst_ref=cells_in.at[slot],
            send_sem=cell_send_sem.at[peer],
            recv_sem=cell_recv_sem.at[slot],
            device_id={"row": peer},
        )

    def value_copy(peer, slot):
        return pltpu.make_async_remote_copy(
            src_ref=send.at[peer],
            dst_ref=recv.at[slot],
            send_sem=send_sem.at[peer],
            recv_sem=recv_sem.at[slot],
            device_id={"row": peer},
        )

    spectra = jnp.zeros((rows, per_device), F32)
    for c in range(PIECES):
        if c == PIECES - 1:
            pl.semaphore_wait(barrier, n - 1)

            def send_cells(i, carry):
                cell_copy(lax.rem(me + i, n), me).start()
                return carry

            lax.fori_loop(1, n, send_cells, 0)
            own_cells = pltpu.make_async_copy(cells_out, cells_in.at[me], own_sem.at[0])
            own_cells.start()
        trace_loads[c].wait()
        spectra += lax.dot_general(
            lhs[:, c * piece : (c + 1) * piece],
            traces[c],
            NT_DIMS,
            preferred_element_type=F32,
        )
    send[...] = spectra.reshape(n, channels, per_device).astype(BF)

    def send_values(i, carry):
        value_copy(lax.rem(me + i, n), me).start()
        return carry

    lax.fori_loop(1, n, send_values, 0)
    own_values = pltpu.make_async_copy(send.at[me], recv.at[me], own_sem.at[1])
    own_values.start()

    cell_at = lax.broadcasted_iota(jnp.int32, (SC, per_device), 0)
    stack[...] = jnp.zeros_like(stack)

    def add(sources):
        s_parts, w_parts = [], []
        for src in sources:
            cell = cells_in[src]
            s_parts.append((cell_at == cell // RC).astype(F32).astype(BF))
            r_hot = (cell_at == cell % RC).astype(F32).astype(BF)
            values = recv[src]
            w_parts.append(
                jnp.concatenate(
                    [r_hot * values[m : m + 1, :] for m in range(channels)] + [r_hot],
                    axis=0,
                )
            )
        stack[...] += lax.dot_general(
            jnp.concatenate(s_parts, axis=1),
            jnp.concatenate(w_parts, axis=1),
            NT_DIMS,
            preferred_element_type=F32,
        )

    own_cells.wait()
    own_values.wait()

    def add_step(g, carry):
        sources = [g * GROUP + k for k in range(GROUP)]
        for src in sources:

            @pl.when(src != me)
            def _():
                cell_copy(src, src).wait_recv()
                value_copy(src, src).wait_recv()

        add(sources)
        return carry

    lax.fori_loop(0, n // GROUP, add_step, 0)

    scale = 1.0 / jnp.maximum(stack[:, channels * RC :], 1.0)
    for m in range(channels):
        out_ref[m // 2, m % 2] = stack[:, m * RC : (m + 1) * RC] * scale

    def drain(i, carry):
        peer = lax.rem(me + i, n)
        cell_copy(peer, me).wait_send()
        value_copy(peer, me).wait_send()
        return carry

    lax.fori_loop(1, n, drain, 0)


def local(n, shot_traces, source_cell, receiver_cell, band_order):
    local_traces, samples_count = shot_traces.shape
    band_size = band_order.shape[0]
    own_slots = band_size // n
    rows = 2 * band_size
    channels = 2 * own_slots
    piece = samples_count // PIECES
    table = jnp.asarray(natural_table(samples_count, band_size))
    anywhere = pl.BlockSpec(memory_space=pltpu.HBM)
    return pl.pallas_call(
        functools.partial(kernel, n),
        out_shape=pltpu.VMEM((own_slots, 2, SC, RC), F32),
        in_specs=[anywhere] * 5,
        out_specs=pl.BlockSpec(memory_space=pltpu.VMEM),
        scratch_shapes=[
            pltpu.VMEM((PIECES, local_traces, piece), BF),
            pltpu.VMEM((1, local_traces), jnp.int32),
            pltpu.VMEM((1, local_traces), jnp.int32),
            pltpu.VMEM((1, band_size), jnp.int32),
            pltpu.VMEM((rows, samples_count), BF),
            pltpu.VMEM((rows, samples_count), BF),
            pltpu.VMEM((1, local_traces), jnp.int32),
            pltpu.VMEM((n, 1, local_traces), jnp.int32),
            pltpu.VMEM((n, channels, local_traces), BF),
            pltpu.VMEM((n, channels, local_traces), BF),
            pltpu.VMEM((SC, (channels + 1) * RC), F32),
            pltpu.SemaphoreType.DMA((4,)),
            pltpu.SemaphoreType.DMA((PIECES,)),
            pltpu.SemaphoreType.DMA((n,)),
            pltpu.SemaphoreType.DMA((n,)),
            pltpu.SemaphoreType.DMA((n,)),
            pltpu.SemaphoreType.DMA((n,)),
            pltpu.SemaphoreType.DMA((2,)),
        ],
        compiler_params=pltpu.CompilerParams(
            collective_id=0, has_side_effects=True, vmem_limit_bytes=64 * 1024 * 1024 - 65536 - 1024 * 1024
        ),
    )(
        shot_traces,
        source_cell.reshape(1, local_traces),
        receiver_cell.reshape(1, local_traces),
        band_order.reshape(1, band_size),
        table,
    )


def solution(mesh):
    placed = (P(("band", "row"), None), P(("band", "row")), P(("band", "row")), P("band"))
    return jax.shard_map(
        functools.partial(local, mesh.shape["row"]),
        mesh=mesh,
        in_specs=placed,
        out_specs=P(("band", "row"), None, None, None),
        check_vma=False,
    )
```

```python
import functools
import math

import jax
import jax.numpy as jnp
import ml_dtypes
import numpy as np
from jax import lax
from jax.experimental import pallas as pl
from jax.experimental.pallas import tpu as pltpu
from jax.sharding import PartitionSpec as P

FLO = 64
SC = 128
RC = 128
PIECES = 4
GROUP = 4
BF = jnp.bfloat16
F32 = jnp.float32
NT_DIMS = (((1,), (1,)), ((), ()))
TN_DIMS = (((0,), (0,)), ((), ()))


def natural_table(samples_count, band_size):
    bins = FLO + np.arange(band_size)
    phase = (bins[:, None] * np.arange(samples_count)[None, :]) % samples_count
    angle = 2.0 * math.pi * phase / samples_count
    scale = 1.0 / math.sqrt(samples_count)
    table = np.stack([np.cos(angle) * scale, -np.sin(angle) * scale], axis=1)
    return table.reshape(2 * band_size, samples_count).astype(np.float32).astype(ml_dtypes.bfloat16)


def kernel(
    n,
    traces_hbm,
    source_hbm,
    receiver_hbm,
    order_hbm,
    table_hbm,
    out_ref,
    traces,
    source,
    receiver,
    order,
    table,
    lhs,
    cells_out,
    cells_in,
    send,
    recv,
    stack,
    load_sem,
    traces_sem,
    cell_send_sem,
    cell_recv_sem,
    send_sem,
    recv_sem,
    own_sem,
):
    me = lax.axis_index("row")
    piece = traces.shape[2]
    per_device = traces.shape[1]
    rows, samples_count = table.shape
    channels = send.shape[1]

    def load(at, src, dst):
        return pltpu.make_async_copy(src, dst, load_sem.at[at])

    loads = [
        load(0, source_hbm, source),
        load(1, receiver_hbm, receiver),
        load(2, order_hbm, order),
        load(3, table_hbm, table),
    ]
    for copy in loads:
        copy.start()
    trace_loads = [
        pltpu.make_async_copy(
            traces_hbm.at[:, pl.ds(c * piece, piece)], traces.at[c], traces_sem.at[c]
        )
        for c in range(PIECES)
    ]
    for copy in trace_loads:
        copy.start()

    barrier = pltpu.get_barrier_semaphore()

    def greet(i, carry):
        pl.semaphore_signal(barrier, inc=1, device_id={"row": lax.rem(me + i, n)})
        return carry

    lax.fori_loop(1, n, greet, 0)

    loads[0].wait()
    loads[1].wait()
    cells_out[...] = source[...] * RC + receiver[...]

    loads[2].wait()
    band_size = rows // 2
    spread = (
        lax.broadcasted_iota(jnp.int32, (band_size, rows), 0)
        == lax.broadcasted_iota(jnp.int32, (band_size, rows), 1) // 2
    ).astype(BF)
    bins = jnp.broadcast_to(order[...].astype(F32), (8, band_size)).astype(BF)
    wanted = jnp.dot(bins, spread, preferred_element_type=F32)[0:1]
    part = lax.broadcasted_iota(jnp.int32, (1, rows), 1) % 2
    wanted = 2.0 * wanted + part.astype(F32)
    held = lax.broadcasted_iota(jnp.int32, (rows, rows), 0).astype(F32)
    pick = (held == wanted).astype(F32).astype(BF)
    loads[3].wait()
    for at in range(0, samples_count, 1024):
        cut = pl.ds(at, 1024)
        lhs[:, cut] = lax.dot_general(
            pick, table[:, cut], TN_DIMS, preferred_element_type=F32
        ).astype(BF)

    def cell_copy(peer, slot):
        return pltpu.make_async_remote_copy(
            src_ref=cells_out,
            dst_ref=cells_in.at[slot],
            send_sem=cell_send_sem.at[peer],
            recv_sem=cell_recv_sem.at[slot],
            device_id={"row": peer},
        )

    def value_copy(peer, slot):
        return pltpu.make_async_remote_copy(
            src_ref=send.at[peer],
            dst_ref=recv.at[slot],
            send_sem=send_sem.at[peer],
            recv_sem=recv_sem.at[slot],
            device_id={"row": peer},
        )

    spectra = jnp.zeros((rows, per_device), F32)
    for c in range(PIECES):
        if c == PIECES - 1:
            pl.semaphore_wait(barrier, n - 1)

            def send_cells(i, carry):
                cell_copy(lax.rem(me + i, n), me).start()
                return carry

            lax.fori_loop(1, n, send_cells, 0)
            own_cells = pltpu.make_async_copy(cells_out, cells_in.at[me], own_sem.at[0])
            own_cells.start()
        trace_loads[c].wait()
        spectra += lax.dot_general(
            lhs[:, c * piece : (c + 1) * piece],
            traces[c],
            NT_DIMS,
            preferred_element_type=F32,
        )
    send[...] = spectra.reshape(n, channels, per_device).astype(BF)

    def send_values(i, carry):
        value_copy(lax.rem(me + i, n), me).start()
        return carry

    lax.fori_loop(1, n, send_values, 0)
    own_values = pltpu.make_async_copy(send.at[me], recv.at[me], own_sem.at[1])
    own_values.start()

    cell_at = lax.broadcasted_iota(jnp.int32, (SC, per_device), 0).astype(F32).astype(BF)
    one = jnp.ones((SC, per_device), BF)
    none = jnp.zeros((SC, per_device), BF)
    stack[...] = jnp.zeros_like(stack)

    def add(sources):
        r_parts, w_parts = [], []
        for src in sources:
            cell = cells_in[src]
            r_parts.append(jnp.where(cell_at == (cell % RC).astype(F32).astype(BF), one, none))
            s_hot = jnp.where(cell_at == (cell // RC).astype(F32).astype(BF), one, none)
            values = recv[src]
            w_parts.append(
                jnp.concatenate(
                    [s_hot * values[m : m + 1, :] for m in range(channels)] + [s_hot],
                    axis=0,
                )
            )
        stack[...] += lax.dot_general(
            jnp.concatenate(w_parts, axis=1),
            jnp.concatenate(r_parts, axis=1),
            NT_DIMS,
            preferred_element_type=F32,
        )

    own_cells.wait()
    own_values.wait()

    def add_step(g, carry):
        sources = [g * GROUP + k for k in range(GROUP)]
        for src in sources:

            @pl.when(src != me)
            def _():
                cell_copy(src, src).wait_recv()
                value_copy(src, src).wait_recv()

        add(sources)
        return carry

    lax.fori_loop(0, n // GROUP, add_step, 0)

    scale = 1.0 / jnp.maximum(stack[channels * SC :], 1.0)
    for m in range(channels):
        out_ref[m // 2, m % 2] = stack[m * SC : (m + 1) * SC] * scale

    def drain(i, carry):
        peer = lax.rem(me + i, n)
        cell_copy(peer, me).wait_send()
        value_copy(peer, me).wait_send()
        return carry

    lax.fori_loop(1, n, drain, 0)


def local(n, shot_traces, source_cell, receiver_cell, band_order):
    local_traces, samples_count = shot_traces.shape
    band_size = band_order.shape[0]
    own_slots = band_size // n
    rows = 2 * band_size
    channels = 2 * own_slots
    piece = samples_count // PIECES
    table = jnp.asarray(natural_table(samples_count, band_size))
    anywhere = pl.BlockSpec(memory_space=pltpu.HBM)
    return pl.pallas_call(
        functools.partial(kernel, n),
        out_shape=pltpu.VMEM((own_slots, 2, SC, RC), F32),
        in_specs=[anywhere] * 5,
        out_specs=pl.BlockSpec(memory_space=pltpu.VMEM),
        scratch_shapes=[
            pltpu.VMEM((PIECES, local_traces, piece), BF),
            pltpu.VMEM((1, local_traces), jnp.int32),
            pltpu.VMEM((1, local_traces), jnp.int32),
            pltpu.VMEM((1, band_size), jnp.int32),
            pltpu.VMEM((rows, samples_count), BF),
            pltpu.VMEM((rows, samples_count), BF),
            pltpu.VMEM((1, local_traces), jnp.int32),
            pltpu.VMEM((n, 1, local_traces), jnp.int32),
            pltpu.VMEM((n, channels, local_traces), BF),
            pltpu.VMEM((n, channels, local_traces), BF),
            pltpu.VMEM(((channels + 1) * SC, RC), F32),
            pltpu.SemaphoreType.DMA((4,)),
            pltpu.SemaphoreType.DMA((PIECES,)),
            pltpu.SemaphoreType.DMA((n,)),
            pltpu.SemaphoreType.DMA((n,)),
            pltpu.SemaphoreType.DMA((n,)),
            pltpu.SemaphoreType.DMA((n,)),
            pltpu.SemaphoreType.DMA((2,)),
        ],
        compiler_params=pltpu.CompilerParams(
            collective_id=0, has_side_effects=True, vmem_limit_bytes=64 * 1024 * 1024 - 65536 - 1024 * 1024
        ),
    )(
        shot_traces,
        source_cell.reshape(1, local_traces),
        receiver_cell.reshape(1, local_traces),
        band_order.reshape(1, band_size),
        table,
    )


def solution(mesh):
    placed = (P(("band", "row"), None), P(("band", "row")), P(("band", "row")), P("band"))
    return jax.shard_map(
        functools.partial(local, mesh.shape["row"]),
        mesh=mesh,
        in_specs=placed,
        out_specs=P(("band", "row"), None, None, None),
        check_vma=False,
    )
```

```python
import functools
import math

import jax
import jax.numpy as jnp
import ml_dtypes
import numpy as np
from jax import lax
from jax.experimental import pallas as pl
from jax.experimental.pallas import tpu as pltpu
from jax.sharding import PartitionSpec as P

FLO = 64
SC = 128
RC = 128
PIECES = 4
GROUP = 4
BF = jnp.bfloat16
F32 = jnp.float32
NT_DIMS = (((1,), (1,)), ((), ()))
TN_DIMS = (((0,), (0,)), ((), ()))


def natural_table(samples_count, band_size):
    bins = FLO + np.arange(band_size)
    phase = (bins[:, None] * np.arange(samples_count)[None, :]) % samples_count
    angle = 2.0 * math.pi * phase / samples_count
    scale = 1.0 / math.sqrt(samples_count)
    table = np.stack([np.cos(angle) * scale, -np.sin(angle) * scale], axis=1)
    return table.reshape(2 * band_size, samples_count).astype(np.float32).astype(ml_dtypes.bfloat16)


def kernel(
    n,
    traces_hbm,
    source_hbm,
    receiver_hbm,
    order_hbm,
    table_hbm,
    out_ref,
    traces,
    source,
    receiver,
    order,
    table,
    lhs,
    cells_out,
    cells_in,
    send,
    recv,
    stack,
    load_sem,
    traces_sem,
    cell_send_sem,
    cell_recv_sem,
    send_sem,
    recv_sem,
    own_sem,
):
    me = lax.axis_index("row")
    piece = traces.shape[2]
    per_device = traces.shape[1]
    rows, samples_count = table.shape
    channels = send.shape[1]

    barrier = pltpu.get_barrier_semaphore()

    def greet(i, carry):
        pl.semaphore_signal(barrier, inc=1, device_id={"row": lax.rem(me + i, n)})
        return carry

    lax.fori_loop(1, n, greet, 0)

    def load(at, src, dst):
        return pltpu.make_async_copy(src, dst, load_sem.at[at])

    loads = [
        load(0, source_hbm, source),
        load(1, receiver_hbm, receiver),
        load(2, order_hbm, order),
        load(3, table_hbm, table),
    ]
    for copy in loads[:3]:
        copy.start()
    trace_loads = [
        pltpu.make_async_copy(
            traces_hbm.at[:, pl.ds(c * piece, piece)], traces.at[c], traces_sem.at[c]
        )
        for c in range(PIECES)
    ]
    trace_loads[0].start()
    loads[3].start()
    for copy in trace_loads[1:]:
        copy.start()

    loads[0].wait()
    loads[1].wait()
    cells_out[...] = source[...] * RC + receiver[...]

    loads[2].wait()
    band_size = rows // 2
    spread = (
        lax.broadcasted_iota(jnp.int32, (band_size, rows), 0)
        == lax.broadcasted_iota(jnp.int32, (band_size, rows), 1) // 2
    ).astype(BF)
    bins = jnp.broadcast_to(order[...].astype(F32), (8, band_size)).astype(BF)
    wanted = jnp.dot(bins, spread, preferred_element_type=F32)[0:1]
    part = lax.broadcasted_iota(jnp.int32, (1, rows), 1) % 2
    wanted = 2.0 * wanted + part.astype(F32)
    held = lax.broadcasted_iota(jnp.int32, (rows, rows), 0).astype(F32)
    pick = (held == wanted).astype(F32).astype(BF)
    loads[3].wait()
    for at in range(0, samples_count, 1024):
        cut = pl.ds(at, 1024)
        lhs[:, cut] = lax.dot_general(
            pick, table[:, cut], TN_DIMS, preferred_element_type=F32
        ).astype(BF)

    def cell_copy(peer, slot):
        return pltpu.make_async_remote_copy(
            src_ref=cells_out,
            dst_ref=cells_in.at[slot],
            send_sem=cell_send_sem.at[peer],
            recv_sem=cell_recv_sem.at[slot],
            device_id={"row": peer},
        )

    def value_copy(peer, slot):
        return pltpu.make_async_remote_copy(
            src_ref=send.at[peer],
            dst_ref=recv.at[slot],
            send_sem=send_sem.at[peer],
            recv_sem=recv_sem.at[slot],
            device_id={"row": peer},
        )

    spectra = jnp.zeros((rows, per_device), F32)
    for c in range(PIECES):
        if c == PIECES - 1:
            pl.semaphore_wait(barrier, n - 1)

            def send_cells(i, carry):
                cell_copy(lax.rem(me + i, n), me).start()
                return carry

            lax.fori_loop(1, n, send_cells, 0)
            own_cells = pltpu.make_async_copy(cells_out, cells_in.at[me], own_sem.at[0])
            own_cells.start()
        trace_loads[c].wait()
        spectra += lax.dot_general(
            lhs[:, c * piece : (c + 1) * piece],
            traces[c],
            NT_DIMS,
            preferred_element_type=F32,
        )
    send[...] = spectra.reshape(n, channels, per_device).astype(BF)

    def send_values(i, carry):
        value_copy(lax.rem(me + i, n), me).start()
        return carry

    lax.fori_loop(1, n, send_values, 0)
    own_values = pltpu.make_async_copy(send.at[me], recv.at[me], own_sem.at[1])
    own_values.start()

    cell_at = lax.broadcasted_iota(jnp.int32, (SC, per_device), 0).astype(F32).astype(BF)
    one = jnp.ones((SC, per_device), BF)
    none = jnp.zeros((SC, per_device), BF)
    stack[...] = jnp.zeros_like(stack)

    def add(sources):
        r_parts, w_parts = [], []
        for src in sources:
            cell = cells_in[src]
            r_parts.append(jnp.where(cell_at == (cell % RC).astype(F32).astype(BF), one, none))
            s_hot = jnp.where(cell_at == (cell // RC).astype(F32).astype(BF), one, none)
            values = recv[src]
            w_parts.append(
                jnp.concatenate(
                    [s_hot * values[m : m + 1, :] for m in range(channels)] + [s_hot],
                    axis=0,
                )
            )
        stack[...] += lax.dot_general(
            jnp.concatenate(w_parts, axis=1),
            jnp.concatenate(r_parts, axis=1),
            NT_DIMS,
            preferred_element_type=F32,
        )

    own_cells.wait()
    own_values.wait()

    def add_step(g, carry):
        sources = [g * GROUP + k for k in range(GROUP)]
        for src in sources:

            @pl.when(src != me)
            def _():
                cell_copy(src, src).wait_recv()
                value_copy(src, src).wait_recv()

        add(sources)
        return carry

    lax.fori_loop(0, n // GROUP, add_step, 0)

    scale = 1.0 / jnp.maximum(stack[channels * SC :], 1.0)
    for m in range(channels):
        out_ref[m // 2, m % 2] = stack[m * SC : (m + 1) * SC] * scale

    def drain(i, carry):
        peer = lax.rem(me + i, n)
        cell_copy(peer, me).wait_send()
        value_copy(peer, me).wait_send()
        return carry

    lax.fori_loop(1, n, drain, 0)


def local(n, shot_traces, source_cell, receiver_cell, band_order):
    local_traces, samples_count = shot_traces.shape
    band_size = band_order.shape[0]
    own_slots = band_size // n
    rows = 2 * band_size
    channels = 2 * own_slots
    piece = samples_count // PIECES
    table = jnp.asarray(natural_table(samples_count, band_size))
    anywhere = pl.BlockSpec(memory_space=pltpu.HBM)
    return pl.pallas_call(
        functools.partial(kernel, n),
        out_shape=pltpu.VMEM((own_slots, 2, SC, RC), F32),
        in_specs=[anywhere] * 5,
        out_specs=pl.BlockSpec(memory_space=pltpu.VMEM),
        scratch_shapes=[
            pltpu.VMEM((PIECES, local_traces, piece), BF),
            pltpu.VMEM((1, local_traces), jnp.int32),
            pltpu.VMEM((1, local_traces), jnp.int32),
            pltpu.VMEM((1, band_size), jnp.int32),
            pltpu.VMEM((rows, samples_count), BF),
            pltpu.VMEM((rows, samples_count), BF),
            pltpu.VMEM((1, local_traces), jnp.int32),
            pltpu.VMEM((n, 1, local_traces), jnp.int32),
            pltpu.VMEM((n, channels, local_traces), BF),
            pltpu.VMEM((n, channels, local_traces), BF),
            pltpu.VMEM(((channels + 1) * SC, RC), F32),
            pltpu.SemaphoreType.DMA((4,)),
            pltpu.SemaphoreType.DMA((PIECES,)),
            pltpu.SemaphoreType.DMA((n,)),
            pltpu.SemaphoreType.DMA((n,)),
            pltpu.SemaphoreType.DMA((n,)),
            pltpu.SemaphoreType.DMA((n,)),
            pltpu.SemaphoreType.DMA((2,)),
        ],
        compiler_params=pltpu.CompilerParams(
            collective_id=0, has_side_effects=True, vmem_limit_bytes=64 * 1024 * 1024 - 65536 - 1024 * 1024
        ),
    )(
        shot_traces,
        source_cell.reshape(1, local_traces),
        receiver_cell.reshape(1, local_traces),
        band_order.reshape(1, band_size),
        table,
    )


def solution(mesh):
    placed = (P(("band", "row"), None), P(("band", "row")), P(("band", "row")), P("band"))
    return jax.shard_map(
        functools.partial(local, mesh.shape["row"]),
        mesh=mesh,
        in_specs=placed,
        out_specs=P(("band", "row"), None, None, None),
        check_vma=False,
    )
```

```python
import functools
import math

import jax
import jax.numpy as jnp
import ml_dtypes
import numpy as np
from jax import lax
from jax.experimental import pallas as pl
from jax.experimental.pallas import tpu as pltpu
from jax.sharding import PartitionSpec as P

FLO = 64
SC = 128
RC = 128
PIECES = 4
GROUP = 4
BF = jnp.bfloat16
F32 = jnp.float32
NT_DIMS = (((1,), (1,)), ((), ()))
TN_DIMS = (((0,), (0,)), ((), ()))


def natural_table(samples_count, band_size):
    bins = FLO + np.arange(band_size)
    phase = (bins[:, None] * np.arange(samples_count)[None, :]) % samples_count
    angle = 2.0 * math.pi * phase / samples_count
    scale = 1.0 / math.sqrt(samples_count)
    table = np.stack([np.cos(angle) * scale, -np.sin(angle) * scale], axis=1)
    return table.reshape(2 * band_size, samples_count).astype(np.float32).astype(ml_dtypes.bfloat16)


def kernel(
    n,
    traces_hbm,
    source_hbm,
    receiver_hbm,
    order_hbm,
    table_hbm,
    out_ref,
    traces,
    source,
    receiver,
    order,
    table,
    lhs,
    cells_out,
    cells_in,
    send,
    recv,
    stack,
    load_sem,
    traces_sem,
    cell_send_sem,
    cell_recv_sem,
    send_sem,
    recv_sem,
    own_sem,
):
    me = lax.axis_index("row")
    piece = traces.shape[2]
    per_device = traces.shape[1]
    rows, samples_count = table.shape
    channels = send.shape[1]

    barrier = pltpu.get_barrier_semaphore()

    def greet(i, carry):
        pl.semaphore_signal(barrier, inc=1, device_id={"row": lax.rem(me + i, n)})
        return carry

    lax.fori_loop(1, n, greet, 0)

    def load(at, src, dst):
        return pltpu.make_async_copy(src, dst, load_sem.at[at])

    loads = [
        load(0, source_hbm, source),
        load(1, receiver_hbm, receiver),
        load(2, order_hbm, order),
        load(3, table_hbm, table),
    ]
    for copy in loads[:3]:
        copy.start()
    trace_loads = [
        pltpu.make_async_copy(
            traces_hbm.at[:, pl.ds(c * piece, piece)], traces.at[c], traces_sem.at[c]
        )
        for c in range(PIECES)
    ]
    trace_loads[0].start()
    loads[3].start()
    for copy in trace_loads[1:]:
        copy.start()

    loads[0].wait()
    loads[1].wait()
    cells_out[...] = source[...] * RC + receiver[...]

    loads[2].wait()
    band_size = rows // 2
    spread = (
        lax.broadcasted_iota(jnp.int32, (band_size, rows), 0)
        == lax.broadcasted_iota(jnp.int32, (band_size, rows), 1) // 2
    ).astype(BF)
    bins = jnp.broadcast_to(order[...].astype(F32), (8, band_size)).astype(BF)
    wanted = jnp.dot(bins, spread, preferred_element_type=F32)[0:1]
    part = lax.broadcasted_iota(jnp.int32, (1, rows), 1) % 2
    wanted = 2.0 * wanted + part.astype(F32)
    held = lax.broadcasted_iota(jnp.int32, (rows, rows), 0).astype(F32)
    pick = (held == wanted).astype(F32).astype(BF)
    loads[3].wait()
    for at in range(0, samples_count, 1024):
        cut = pl.ds(at, 1024)
        lhs[:, cut] = lax.dot_general(
            pick, table[:, cut], TN_DIMS, preferred_element_type=F32
        ).astype(BF)

    def cell_copy(peer, slot):
        return pltpu.make_async_remote_copy(
            src_ref=cells_out,
            dst_ref=cells_in.at[slot],
            send_sem=cell_send_sem.at[peer],
            recv_sem=cell_recv_sem.at[slot],
            device_id={"row": peer},
        )

    def value_copy(peer, slot):
        return pltpu.make_async_remote_copy(
            src_ref=send.at[peer],
            dst_ref=recv.at[slot],
            send_sem=send_sem.at[peer],
            recv_sem=recv_sem.at[slot],
            device_id={"row": peer},
        )

    spectra = jnp.zeros((rows, per_device), F32)
    for c in range(PIECES):
        if c == PIECES - 1:
            pl.semaphore_wait(barrier, n - 1)

            def send_cells(i, carry):
                cell_copy(lax.rem(me + i, n), me).start()
                return carry

            lax.fori_loop(1, n, send_cells, 0)
            own_cells = pltpu.make_async_copy(cells_out, cells_in.at[me], own_sem.at[0])
            own_cells.start()
        trace_loads[c].wait()
        spectra += lax.dot_general(
            lhs[:, c * piece : (c + 1) * piece],
            traces[c],
            NT_DIMS,
            preferred_element_type=F32,
        )
    send[...] = spectra.reshape(n, channels, per_device).astype(BF)

    def send_values(i, carry):
        value_copy(lax.rem(me + i, n), me).start()
        return carry

    lax.fori_loop(1, n, send_values, 0)
    own_values = pltpu.make_async_copy(send.at[me], recv.at[me], own_sem.at[1])
    own_values.start()

    cell_at = lax.broadcasted_iota(jnp.int32, (SC, per_device), 0).astype(F32).astype(BF)
    one = jnp.ones((SC, per_device), BF)
    none = jnp.zeros((SC, per_device), BF)
    stack[...] = jnp.zeros_like(stack)

    def add(sources):
        r_parts, w_parts = [], []
        for src in sources:
            cell = cells_in[src]
            r_parts.append(jnp.where(cell_at == (cell % RC).astype(F32).astype(BF), one, none))
            s_hot = jnp.where(cell_at == (cell // RC).astype(F32).astype(BF), one, none)
            values = recv[src]
            w_parts.append(
                jnp.concatenate(
                    [s_hot * values[m : m + 1, :] for m in range(channels)] + [s_hot],
                    axis=0,
                )
            )
        stack[...] += sum(
            lax.dot_general(w, r, NT_DIMS, preferred_element_type=F32)
            for w, r in zip(w_parts, r_parts)
        )

    own_cells.wait()
    own_values.wait()

    def add_step(g, carry):
        sources = [g * GROUP + k for k in range(GROUP)]
        for src in sources:

            @pl.when(src != me)
            def _():
                cell_copy(src, src).wait_recv()
                value_copy(src, src).wait_recv()

        add(sources)
        return carry

    lax.fori_loop(0, n // GROUP, add_step, 0)

    scale = 1.0 / jnp.maximum(stack[channels * SC :], 1.0)
    for m in range(channels):
        out_ref[m // 2, m % 2] = stack[m * SC : (m + 1) * SC] * scale

    def drain(i, carry):
        peer = lax.rem(me + i, n)
        cell_copy(peer, me).wait_send()
        value_copy(peer, me).wait_send()
        return carry

    lax.fori_loop(1, n, drain, 0)


def local(n, shot_traces, source_cell, receiver_cell, band_order):
    local_traces, samples_count = shot_traces.shape
    band_size = band_order.shape[0]
    own_slots = band_size // n
    rows = 2 * band_size
    channels = 2 * own_slots
    piece = samples_count // PIECES
    table = jnp.asarray(natural_table(samples_count, band_size))
    anywhere = pl.BlockSpec(memory_space=pltpu.HBM)
    return pl.pallas_call(
        functools.partial(kernel, n),
        out_shape=pltpu.VMEM((own_slots, 2, SC, RC), F32),
        in_specs=[anywhere] * 5,
        out_specs=pl.BlockSpec(memory_space=pltpu.VMEM),
        scratch_shapes=[
            pltpu.VMEM((PIECES, local_traces, piece), BF),
            pltpu.VMEM((1, local_traces), jnp.int32),
            pltpu.VMEM((1, local_traces), jnp.int32),
            pltpu.VMEM((1, band_size), jnp.int32),
            pltpu.VMEM((rows, samples_count), BF),
            pltpu.VMEM((rows, samples_count), BF),
            pltpu.VMEM((1, local_traces), jnp.int32),
            pltpu.VMEM((n, 1, local_traces), jnp.int32),
            pltpu.VMEM((n, channels, local_traces), BF),
            pltpu.VMEM((n, channels, local_traces), BF),
            pltpu.VMEM(((channels + 1) * SC, RC), F32),
            pltpu.SemaphoreType.DMA((4,)),
            pltpu.SemaphoreType.DMA((PIECES,)),
            pltpu.SemaphoreType.DMA((n,)),
            pltpu.SemaphoreType.DMA((n,)),
            pltpu.SemaphoreType.DMA((n,)),
            pltpu.SemaphoreType.DMA((n,)),
            pltpu.SemaphoreType.DMA((2,)),
        ],
        compiler_params=pltpu.CompilerParams(
            collective_id=0, has_side_effects=True, vmem_limit_bytes=64 * 1024 * 1024 - 65536 - 1024 * 1024
        ),
    )(
        shot_traces,
        source_cell.reshape(1, local_traces),
        receiver_cell.reshape(1, local_traces),
        band_order.reshape(1, band_size),
        table,
    )


def solution(mesh):
    placed = (P(("band", "row"), None), P(("band", "row")), P(("band", "row")), P("band"))
    return jax.shard_map(
        functools.partial(local, mesh.shape["row"]),
        mesh=mesh,
        in_specs=placed,
        out_specs=P(("band", "row"), None, None, None),
        check_vma=False,
    )
```
